32 devices in a mesh: gx: 4 (over y, x), gy: 8 (over z, core).
Axes of the slice: x: 2, y: 2, z: 4, core: 2. Of those that a mesh axis runs over, the one named last changes fastest.
Arguments:
- fine_nodes: bfloat16 [65536, 256], P(('gx', 'gy')), may hold values from -6 to 6
- fine_weights: bfloat16 [6, 256, 256], replicated, may hold values from -0.375 to 0.375
- coarse_weights: bfloat16 [6, 256, 256], replicated, may hold values from -0.375 to 0.375
- top_weights: bfloat16 [6, 256, 256], replicated, may hold values from -0.375 to 0.375
- gains: float32 [3, 256], replicated, may hold values from 0.1 to 1.9
- send_list: int32 [4, 8, 4, 512], P('gx', 'gy'), may hold values from 0 to 2047
- fine_sender: int32 [4, 8, 8192], P('gx', 'gy'), may hold values from 0 to 4095, as said below
- fine_receiver: int32 [4, 8, 8192], P('gx', 'gy'), may hold values from 0 to 2048, as said below
- pool_owner: int32 [65536, 1], P(('gx', 'gy')), may hold values from 0 to 3; in each aligned block of 2048 rows (0 to 2047, 2048 to 4095, ...) at most 1024 rows name the same one
- pool_local: int32 [65536], P(('gx', 'gy')), may hold values from 0 to 255
- coarse_sender: int32 [8, 4096], P('gy', 'gx'), may hold values from 0 to 1023
- coarse_receiver: int32 [8, 4096], P('gy', 'gx'), may hold values from 0 to 255
- top_parent: int32 [8, 1024], P('gy', 'gx'), may hold values from 0 to 127
- top_sender: int32 [8, 512], P('gy'), may hold values from 0 to 127
- top_receiver: int32 [8, 512], P('gy'), may hold values from 0 to 127
Outputs:
- fine_state: bfloat16 [65536, 256], P(('gx', 'gy'))
- coarse_state: bfloat16 [8, 1024, 256], P('gy', 'gx')
The draws below stay inside these ranges and needn't reach their ends.
Inputs may be any that keep to these rules, and one draw needn't show every extreme that they name: `fine_sender`: values below 2048 name the device's own nodes; larger values name a halo row of a neighbour that exists. `fine_receiver`: 2048 marks an empty slot; a device's live slots come first, and some device has no empty slot. `pool_owner`: among the rows of one device no member is named more than 1024 times.
All inputs are finite; a program needn't handle non-finite values.
Results may differ from the reference program's by a relative error of at most 0.015.
Values may be sent and summed in bfloat16 or wider, within the bound.
No kernel may reach another device: no remote copies, remote signals or barrier semaphores. Data moves between devices by JAX's collectives and lax.ppermute only.
A program may use at most 64 MiB of HBM per device.

```python
import math
import jax
import jax.numpy as jnp
import numpy as np
from jax import lax

H = 256
NF_DEV = 2048
HALO = 512
NF_ALL = 65536
EF_DEV = 8192
NC_DEV = 256
EC_DEV = 1024
NC_SUB = 1024
NT = 128
ET = 512
CAP = 1024
N_GX = 4
N_GY = 8


def draw_fine_sender(key, part):
    extent = (N_GX, N_GY, EF_DEV)
    key_own, key_side, key_halo, key_pick = jax.random.split(jax.random.fold_in(key, 11), 4)
    own_rows = jax.random.randint(key_own, extent, 0, NF_DEV)
    direction = jax.random.randint(key_side, extent, 0, 4)
    halo_row = jax.random.randint(key_halo, extent, 0, HALO)
    remote = jax.random.randint(key_pick, extent, 0, 4) == 0
    dev_row = lax.broadcasted_iota(jnp.int32, extent, 0)
    dev_col = lax.broadcasted_iota(jnp.int32, extent, 1)
    exists = jnp.where(direction == 0, dev_row > 0, jnp.where(direction == 1, dev_row < N_GX - 1, jnp.where(direction == 2, dev_col > 0, dev_col < N_GY - 1)))
    return jnp.where(remote & exists, NF_DEV + direction * HALO + halo_row, own_rows).astype(jnp.int32)


def draw_fine_receiver(key, part):
    extent = (N_GX, N_GY, EF_DEV)
    key_live, key_full, key_node = jax.random.split(jax.random.fold_in(key, 23), 3)
    live = jax.random.randint(key_live, (N_GX, N_GY), EF_DEV // 2, EF_DEV + 1)
    full_device = jax.random.randint(key_full, (), 0, N_GX * N_GY)
    device = lax.broadcasted_iota(jnp.int32, (N_GX, N_GY), 0) * N_GY + lax.broadcasted_iota(jnp.int32, (N_GX, N_GY), 1)
    live = jnp.where(device == full_device, EF_DEV, live)
    targets = jax.random.randint(key_node, extent, 0, NF_DEV)
    slot = lax.broadcasted_iota(jnp.int32, extent, 2)
    return jnp.where(slot < live[:, :, None], targets, NF_DEV).astype(jnp.int32)


def draw_coarse_sender(key, part):
    extent = (N_GY, N_GX * EC_DEV)
    key_near, key_far, key_pick = jax.random.split(jax.random.fold_in(key, 37), 3)
    owner = lax.broadcasted_iota(jnp.int32, extent, 1) // EC_DEV
    nearby = owner * NC_DEV + jax.random.randint(key_near, extent, 0, NC_DEV)
    anywhere = jax.random.randint(key_far, extent, 0, NC_SUB)
    choose_near = jax.random.randint(key_pick, extent, 0, 2) == 0
    return jnp.where(choose_near, nearby, anywhere).astype(jnp.int32)


def place_ends(drawn, key, least, largest):
    index_at = [jax.random.randint(jax.random.fold_in(key, axis), (), 0, length) for axis, length in enumerate(drawn.shape)]
    widest = drawn.shape.index(max(drawn.shape))
    beside = index_at[:widest] + [(index_at[widest] + 1) % drawn.shape[widest]] + index_at[widest + 1:]
    return drawn.at[tuple(index_at)].set(least).at[tuple(beside)].set(largest)


def level_of(own_key, shape, shards, smallest, high):
    level = 1.0
    for dim, parts in shards:
        heights = jax.random.uniform(jax.random.fold_in(jax.random.fold_in(own_key, 6), dim), (parts,), jnp.float32, smallest / len(shards), high / len(shards))
        level = level * jnp.repeat(jnp.exp(heights), shape[dim] // parts).reshape((-1,) + (1,) * (len(shape) - 1 - dim))
    return level


def rank_table(amount, lean):
    portions = [(1 << 20) // math.isqrt(rank ** lean) + 1 for rank in range(1, amount + 1)]
    deviation = 1 + sum(portions) // (1 << 30)
    return np.cumsum(np.array([max(1, weight // deviation) for weight in portions]))


def ranked(stream_key, shape, number_of, slope):
    table = rank_table(number_of, slope)
    ticket = jax.random.randint(jax.random.fold_in(stream_key, 1), shape, 0, int(table[number_of - 1]))
    grade = jnp.searchsorted(jnp.asarray(table, jnp.int32), ticket, side="right")
    return jax.random.permutation(jax.random.fold_in(stream_key, 2), number_of)[grade].astype(jnp.int32)


def assign_block(stream_key, own, number, rows, count, top, limit, skew):
    sequence = jax.random.permutation(stream_key, count)
    heavy_load, usual = shares(count, rows * top, limit, skew, True), shares(count, rows * top, limit, skew, False)
    places = jnp.arange(count)

    def named(tallies, turn):
        used = int((tallies > 0).sum())
        fixed = max(1, used // 4)
        moved = fixed + (places - fixed + turn * (used - fixed)) % max(1, count - fixed)
        return jnp.zeros((count,), jnp.int32).at[sequence[jnp.where(places < fixed, places, moved)]].set(jnp.asarray(tallies, jnp.int32))

    tallies = jnp.where(number % 4 == 0, named(heavy_load, number // 4), named(usual, number - number // 4 - 1))
    mixed = jax.random.permutation(jax.random.fold_in(own, 3), count)
    donor, receiver = mixed[0:count // 2 * 2:2], mixed[1:count // 2 * 2:2]
    room = jnp.minimum(tallies[donor] - 1, limit - tallies[receiver]) // 2
    room = jnp.where((donor == sequence[0]) | (receiver == sequence[0]) | (tallies[receiver] == 0), 0, jnp.maximum(room, 0))
    moved = jax.random.randint(jax.random.fold_in(own, 4), (count // 2,), 0, 1 << 20) % (room + 1)
    tallies = tallies.at[donor].add(-moved).at[receiver].add(moved)
    members = jnp.searchsorted(jnp.cumsum(tallies), jnp.arange(rows * top), side="right").astype(jnp.int32)
    listing = members.reshape(top, rows).T
    listing = listing[jax.random.permutation(jax.random.fold_in(own, 1), rows)]
    turn = jax.random.randint(jax.random.fold_in(own, 2), (rows, 1), 0, top)
    return jnp.take_along_axis(listing, (jnp.arange(top)[None, :] + turn) % top, axis=1)


def shares(amount, total, most, lean, full):
    weights = [(1 << 20) // math.isqrt(grade ** lean) + 1 for grade in range(1, amount + 1)]
    largest = most if full else min(most, max(-(-total // amount), total * weights[0] // sum(weights)))
    least = 1 if total - largest >= amount - 1 else 0
    counts, surplus = [largest] + [least] * (amount - 1), total - largest - least * (amount - 1)
    while surplus > 0:
        candidates = [i for i in range(1, amount) if counts[i] < largest] or [i for i in range(1, amount) if counts[i] < most]
        mass, remaining = sum([weights[i] for i in candidates]), surplus
        for i in candidates:
            addition = min(most - counts[i], max(1, remaining * weights[i] // mass), surplus)
            counts[i] = counts[i] + addition
            surplus = surplus - addition
    return np.array(counts)


def noise(key, shape, scale, most, pieces=(), held_as=jnp.bfloat16):
    values = scale * jax.random.normal(key, shape, jnp.float32)
    if pieces:
        values = values * level_of(key, shape, pieces, -0.22, 0.18)
    return jnp.clip(values, -most, most).astype(held_as)


def setup_inputs(seed: int = 0) -> dict:
    arg_keys = jax.random.split(jax.random.key(seed), 16)
    fine_nodes = noise(arg_keys[0], (NF_ALL, H), 1.0, 6.0, ((0, 32),))
    fine_weights = noise(arg_keys[1], (6, H, H), H ** -0.5, 0.375)
    coarse_weights = noise(arg_keys[2], (6, H, H), H ** -0.5, 0.375)
    top_weights = noise(arg_keys[3], (6, H, H), H ** -0.5, 0.375)
    gains = jnp.clip(1.0 + 0.18 * jax.random.normal(arg_keys[4], (3, H), jnp.float32), 0.1, 1.9)
    send_list = place_ends(jax.random.randint(arg_keys[5], (N_GX, N_GY, 4, HALO), 0, NF_DEV), jax.random.fold_in(arg_keys[5], 1), 0, NF_DEV - 1).astype(jnp.int32)
    fine_sender = draw_fine_sender(jax.random.fold_in(arg_keys[15], 71), 0)
    fine_receiver = draw_fine_receiver(jax.random.fold_in(arg_keys[15], 71), 0)
    pool_owner_keys = jax.random.split(jax.random.fold_in(arg_keys[8], 1), NF_ALL // NF_DEV)
    pool_owner_turns = jax.random.permutation(jax.random.fold_in(arg_keys[8], 3), NF_ALL // NF_DEV)
    pool_owner = jax.vmap(lambda own, number: assign_block(jax.random.fold_in(arg_keys[8], 2), own, number, NF_DEV, N_GX, 1, CAP, 2))(pool_owner_keys, pool_owner_turns).reshape((NF_ALL, 1))
    pool_local = place_ends(jax.random.randint(arg_keys[9], (NF_ALL,), 0, NC_DEV), jax.random.fold_in(arg_keys[9], 1), 0, NC_DEV - 1).astype(jnp.int32)
    coarse_sender = draw_coarse_sender(jax.random.fold_in(arg_keys[15], 71), 0)
    coarse_receiver = place_ends(jax.random.randint(arg_keys[11], (N_GY, N_GX * EC_DEV), 0, NC_DEV), jax.random.fold_in(arg_keys[11], 1), 0, NC_DEV - 1).astype(jnp.int32)
    top_parent = place_ends(ranked(arg_keys[12], (N_GY, NC_SUB), NT, 1), jax.random.fold_in(arg_keys[12], 3), 0, NT - 1).astype(jnp.int32)
    top_sender = place_ends(jax.random.randint(arg_keys[13], (N_GY, ET), 0, NT), jax.random.fold_in(arg_keys[13], 1), 0, NT - 1).astype(jnp.int32)
    top_receiver = place_ends(jax.random.randint(arg_keys[14], (N_GY, ET), 0, NT), jax.random.fold_in(arg_keys[14], 1), 0, NT - 1).astype(jnp.int32)
    return {"fine_nodes": fine_nodes, "fine_weights": fine_weights, "coarse_weights": coarse_weights, "top_weights": top_weights, "gains": gains, "send_list": send_list, "fine_sender": fine_sender, "fine_receiver": fine_receiver, "pool_owner": pool_owner, "pool_local": pool_local, "coarse_sender": coarse_sender, "coarse_receiver": coarse_receiver, "top_parent": top_parent, "top_sender": top_sender, "top_receiver": top_receiver}


def project(states, weights):
    sender_term = jnp.dot(states, weights[0], preferred_element_type=jnp.float32).astype(jnp.bfloat16)
    receiver_term = jnp.dot(states, weights[1], preferred_element_type=jnp.float32).astype(jnp.bfloat16)
    return (sender_term, receiver_term)

def gather_messages(fetch, receiver_term, receivers, weight_out, count, most):
    edges = receivers.shape[0]
    block = math.gcd(edges, most)
    width = receiver_term.shape[1]

    def advance(summed, turn):
        begin = (turn * block).astype(jnp.int32)
        targets = lax.dynamic_slice_in_dim(receivers, begin, block)
        before = fetch(begin, block) + jnp.take(receiver_term, jnp.minimum(targets, count - 1), axis=0).astype(jnp.float32)
        hidden = jax.nn.silu(before).astype(jnp.bfloat16)
        message = jnp.dot(hidden, weight_out, preferred_element_type=jnp.float32)
        return (summed.at[targets].add(message, mode='drop'), None)
    turns = jnp.arange(edges // block, dtype=jnp.int32)
    summed, unused = lax.scan(advance, jnp.zeros((count, width), jnp.float32), turns)
    return summed

def update_nodes(states, aggregate, weights, gain):
    merged = jnp.dot(states, weights[3], preferred_element_type=jnp.float32)
    merged = merged + jnp.dot(aggregate.astype(jnp.bfloat16), weights[4], preferred_element_type=jnp.float32)
    inner = jax.nn.silu(merged).astype(jnp.bfloat16)
    output = jnp.dot(inner, weights[5], preferred_element_type=jnp.float32)
    centred = output - lax.optimization_barrier(jnp.mean(output, axis=1, keepdims=True))
    spread = lax.optimization_barrier(jnp.mean(centred * centred, axis=1, keepdims=True))
    return (states.astype(jnp.float32) + gain * centred * lax.rsqrt(spread + 1e-05)).astype(jnp.bfloat16)

def run_layer(states, senders, receivers, weights, gain, most):
    sender_term, receiver_term = project(states, weights)
    count = states.shape[0]

    def fetch(begin, rows):
        picked = lax.dynamic_slice_in_dim(senders, begin, rows)
        return jnp.take(sender_term, picked, axis=0).astype(jnp.float32)
    aggregate = gather_messages(fetch, receiver_term, receivers, weights[2], count, most)
    return update_nodes(states, aggregate, weights, gain)

def reference(fine_nodes, fine_weights, coarse_weights, top_weights, gains, send_list, fine_sender, fine_receiver, pool_owner, pool_local, coarse_sender, coarse_receiver, top_parent, top_sender, top_receiver):
    extent = (N_GX, N_GY, EF_DEV)
    dev_row = lax.broadcasted_iota(jnp.int32, extent, 0)
    dev_col = lax.broadcasted_iota(jnp.int32, extent, 1)
    device = dev_row * N_GY + dev_col
    offset = fine_sender - NF_DEV
    direction = jnp.clip(offset // HALO, 0, 3).astype(jnp.int32)
    halo_row = jnp.clip(offset % HALO, 0, HALO - 1).astype(jnp.int32)
    row_step = jnp.array([-1, 1, 0, 0], jnp.int32)[direction]
    col_step = jnp.array([0, 0, -1, 1], jnp.int32)[direction]
    from_row = jnp.clip(dev_row + row_step, 0, N_GX - 1)
    from_col = jnp.clip(dev_col + col_step, 0, N_GY - 1)
    listed = send_list[from_row, from_col, direction, halo_row]
    fine_senders = jnp.where(fine_sender < NF_DEV, device * NF_DEV + fine_sender, (from_row * N_GY + from_col) * NF_DEV + listed).astype(jnp.int32)
    fine_receivers = jnp.where(fine_receiver < NF_DEV, device * NF_DEV + fine_receiver, NF_ALL).astype(jnp.int32)
    fine_one = run_layer(fine_nodes, fine_senders.reshape(-1), fine_receivers.reshape(-1), fine_weights, gains[0], 65536)
    fine_ids = jnp.arange(NF_ALL, dtype=jnp.int32)
    subgroup = fine_ids // NF_DEV % N_GY
    coarse_index = (subgroup * NC_SUB + pool_owner[:, 0] * NC_DEV + pool_local).astype(jnp.int32)
    coarse_count = N_GY * NC_SUB
    coarse_sum = jnp.zeros((coarse_count, H), jnp.float32).at[coarse_index].add(fine_one.astype(jnp.float32))
    child_count = jnp.zeros((coarse_count,), jnp.float32).at[coarse_index].add(1.0)
    coarse_zero = (coarse_sum / jnp.maximum(child_count, 1.0)[:, None]).astype(jnp.bfloat16)
    coarse_extent = (N_GY, N_GX * EC_DEV)
    coarse_group = lax.broadcasted_iota(jnp.int32, coarse_extent, 0)
    coarse_column = lax.broadcasted_iota(jnp.int32, coarse_extent, 1)
    coarse_senders = (coarse_group * NC_SUB + coarse_sender).astype(jnp.int32)
    coarse_receivers = (coarse_group * NC_SUB + coarse_column // EC_DEV * NC_DEV + coarse_receiver).astype(jnp.int32)
    coarse_one = run_layer(coarse_zero, coarse_senders.reshape(-1), coarse_receivers.reshape(-1), coarse_weights, gains[1], 65536)
    parent_group = lax.broadcasted_iota(jnp.int32, (N_GY, NC_SUB), 0)
    top_index = (parent_group * NT + top_parent).reshape(-1).astype(jnp.int32)
    top_sum = jnp.zeros((N_GY * NT, H), jnp.float32).at[top_index].add(coarse_one.astype(jnp.float32))
    top_count = jnp.zeros((N_GY * NT,), jnp.float32).at[top_index].add(1.0)
    top_zero = (top_sum / jnp.maximum(top_count, 1.0)[:, None]).astype(jnp.bfloat16)
    top_group = lax.broadcasted_iota(jnp.int32, (N_GY, ET), 0)
    top_senders = (top_group * NT + top_sender).reshape(-1).astype(jnp.int32)
    top_receivers = (top_group * NT + top_receiver).reshape(-1).astype(jnp.int32)
    top_one = run_layer(top_zero, top_senders, top_receivers, top_weights, gains[2], 65536)
    coarse_two = (coarse_one.astype(jnp.float32) + jnp.take(top_one, top_index, axis=0).astype(jnp.float32)).astype(jnp.bfloat16)
    fine_state = (fine_one.astype(jnp.float32) + jnp.take(coarse_two, coarse_index, axis=0).astype(jnp.float32)).astype(jnp.bfloat16)
    return (fine_state, coarse_two.reshape(N_GY, NC_SUB, H))
```

```python
import functools

import jax
import jax.numpy as jnp
from jax import lax
from jax.experimental import pallas as pl
from jax.experimental.pallas import tpu as pltpu
from jax.sharding import PartitionSpec as P

F32 = jnp.float32
BF16 = jnp.bfloat16
LANES = 128
PAD = 8
CHUNK = 512
ROWS = 256
VMEM_LIMIT = 56 << 20

SMEM_SPEC = pl.BlockSpec(memory_space=pltpu.SMEM)
VMEM_SPEC = pl.BlockSpec(memory_space=pltpu.VMEM)


def shifted(block, axis, distance, wrap):
    count = lax.axis_size(axis)
    route = []
    for i in range(count):
        j = i + distance
        if wrap:
            route.append((i, j % count))
        elif 0 <= j < count:
            route.append((i, j))
    return lax.ppermute(block, axis, route)


def dot(a, b):
    return jnp.dot(a, b, preferred_element_type=F32)


def silu(v):
    return (0.5 * v) * (1.0 + jnp.tanh(0.5 * v))


def put_rows(table, stride, begin, rows, values):
    table[begin : begin + rows, :] = values[:, :LANES]
    table[stride + begin : stride + begin + rows, :] = values[:, LANES:]


def project_into(table, stride, begin, states, weight):
    rows = states.shape[0]
    step = min(rows, 512)
    for at in range(0, rows, step):
        term = dot(states[at : at + step, :], weight).astype(BF16).astype(F32)
        put_rows(table, stride, begin + at, step, term)


def selection(indices, begin, rows):
    columns = indices.shape[1]
    number = lax.broadcasted_iota(jnp.int32, (rows, columns), 0) + begin
    return jnp.where(number == indices, 1.0, 0.0).astype(BF16)


def gather_chunk(c, chunk, s_ref, r_ref, ts, s_stride, tr, r_stride, buf):
    base = c * chunk
    for j in range(chunk):
        s = s_ref[base + j]
        r = r_ref[base + j]
        buf[pl.ds(j, 2, stride=chunk + PAD), :] = (
            ts[pl.ds(s, 2, stride=s_stride), :] + tr[pl.ds(r, 2, stride=r_stride), :]
        )


def edge_sums(nodes, edges, s_ref, r_ref, rv_ref, ts, s_stride, tr, r_stride, buf, hid, acc):
    chunk = rv_ref.shape[1]
    turns = edges // chunk
    block = min(ROWS, nodes)
    acc[0:nodes, :] = jnp.zeros((nodes, 2 * LANES), F32)

    def gather(c):
        gather_chunk(c, chunk, s_ref, r_ref, ts, s_stride, tr, r_stride, buf)

    def activate():
        hid[0:chunk, :LANES] = silu(buf[0:chunk, :]).astype(BF16)
        hid[0:chunk, LANES:] = silu(buf[chunk + PAD : 2 * chunk + PAD, :]).astype(BF16)

    def add(c):
        targets = rv_ref[pl.ds(c, 1), :]
        hidden = hid[0:chunk, :]
        for at in range(0, nodes, block):
            acc[at : at + block, :] += dot(selection(targets, at, block), hidden)

    gather(0)

    def turn(c, carry):
        activate()
        gather(c + 1)
        add(c)
        return carry

    if turns > 1:
        lax.fori_loop(0, turns - 1, turn, 0)
    activate()
    add(turns - 1)


def updated(states, summed, w_ref, gain):
    aggregate = dot(summed.astype(BF16), w_ref[2]).astype(BF16)
    inner = silu(dot(states, w_ref[3]) + dot(aggregate, w_ref[4])).astype(BF16)
    output = dot(inner, w_ref[5])
    centred = output - jnp.mean(output, axis=1, keepdims=True)
    spread = jnp.mean(centred * centred, axis=1, keepdims=True)
    return states.astype(F32) + gain * centred * lax.rsqrt(spread + 1e-05)


def halo_kernel(l_ref, nodes, *refs):
    outs, (table, buf) = refs[:4], refs[4:]
    rows = nodes.shape[0]
    listed = outs[0].shape[0]
    unroll = 64
    put_rows(table, rows + PAD, 0, rows, nodes[...].astype(F32))
    for d in range(4):

        def some(c, carry):
            base = pl.multiple_of(c * unroll, unroll)
            for j in range(unroll):
                i = l_ref[d * listed + base + j]
                buf[pl.ds(base + j, 2, stride=listed + PAD), :] = table[
                    pl.ds(i, 2, stride=rows + PAD), :
                ]
            return carry

        lax.fori_loop(0, listed // unroll, some, 0)
        outs[d][:, :LANES] = buf[0:listed, :].astype(BF16)
        outs[d][:, LANES:] = buf[listed + PAD : 2 * listed + PAD, :].astype(BF16)


def count_kernel(members, p_ref, out):
    size = out.shape[1]
    eye = lax.broadcasted_iota(jnp.int32, (size, size), 0) == lax.broadcasted_iota(
        jnp.int32, (size, size), 1
    )
    parents = p_ref[...]
    for d in range(members):
        chosen = jnp.where(
            lax.broadcasted_iota(jnp.int32, (size, parents.shape[1]), 0) + d * size == parents,
            1.0,
            0.0,
        )
        column = jnp.sum(chosen, axis=1, keepdims=True)
        row = jnp.sum(jnp.where(eye, column, 0.0), axis=0, keepdims=True)
        out[d : d + 1, :] = row.astype(jnp.int32)


def fine_kernel(members, s_ref, r_ref, rv_ref, p_ref, nodes, h0, h1, h2, h3, w_ref, g_ref, *refs):
    one, parts = refs[0], refs[1 : 1 + members]
    ts, tr, buf, hid, acc = refs[1 + members :]
    count = nodes.shape[0]
    edges = s_ref.shape[0]
    listed = h0.shape[0]
    s_stride = count + 4 * listed + PAD
    r_stride = count + PAD
    project_into(ts, s_stride, 0, nodes, w_ref[0])
    for d, halo in enumerate((h0, h1, h2, h3)):
        project_into(ts, s_stride, count + d * listed, halo, w_ref[0])
    project_into(tr, r_stride, 0, nodes, w_ref[1])
    put_rows(tr, r_stride, count, PAD, jnp.zeros((PAD, 2 * LANES), F32))
    edge_sums(count, edges, s_ref, r_ref, rv_ref, ts, s_stride, tr, r_stride, buf, hid, acc)
    gain = g_ref[0:1, :]
    step = 512
    for at in range(0, count, step):
        rows = slice(at, at + step)
        one[rows, :] = updated(nodes[rows, :], acc[rows, :], w_ref, gain).astype(BF16)
    parents = p_ref[...]
    size = parts[0].shape[0]
    for d in range(members):
        parts[d][...] = dot(selection(parents, d * size, size), one[...]).astype(BF16)


def mean_kernel(members, c_ref, *refs):
    pieces, out = refs[:members], refs[members]
    size = out.shape[0]
    eye = lax.broadcasted_iota(jnp.int32, (size, size), 0) == lax.broadcasted_iota(
        jnp.int32, (size, size), 1
    )
    total = pieces[0][...].astype(F32)
    for piece in pieces[1:]:
        total = total + piece[...].astype(F32)
    children = jnp.sum(c_ref[...].astype(F32), axis=0, keepdims=True)
    column = jnp.sum(jnp.where(eye, children, 0.0), axis=1, keepdims=True)
    out[...] = (total / jnp.maximum(column, 1.0)).astype(BF16)


def turned(row):
    n = row.shape[1]
    return jnp.concatenate(
        [
            jnp.transpose(jnp.broadcast_to(row[:, at : at + LANES], (LANES, LANES)))
            for at in range(0, n, LANES)
        ],
        axis=0,
    )


def picks(row, columns):
    column = turned(row)
    lane = lax.broadcasted_iota(jnp.int32, column.shape, 1)
    return jnp.concatenate(
        [
            jnp.where(column == lane + at, 1.0, 0.0).astype(BF16)
            for at in range(0, columns, LANES)
        ],
        axis=1,
    )


def upper_kernel(
    members,
    cs_ref,
    cr_ref,
    crv_ref,
    ts_ref,
    tr_ref,
    trv_ref,
    tp_ref,
    p_ref,
    fine,
    cw_ref,
    tw_ref,
    g_ref,
    *refs,
):
    pieces = refs[:members]
    fine_out, coarse_out = refs[members : members + 2]
    ts, tr, buf, hid, acc, zero, one = refs[members + 2 :]
    size = pieces[0].shape[0]
    count = size * members
    tops = count // 8
    stride = count + PAD
    for d in range(members):
        zero[d * size : (d + 1) * size, :] = pieces[d][...]
    project_into(ts, stride, 0, zero, cw_ref[0])
    project_into(tr, stride, 0, zero, cw_ref[1])
    edge_sums(
        count, cs_ref.shape[0], cs_ref, cr_ref, crv_ref, ts, stride, tr, stride, buf, hid, acc
    )
    gain = g_ref[1:2, :]
    step = min(count, 512)
    for at in range(0, count, step):
        rows = slice(at, at + step)
        one[rows, :] = updated(zero[rows, :], acc[rows, :], cw_ref, gain).astype(BF16)
    chosen = jnp.where(
        lax.broadcasted_iota(jnp.int32, (tops, count), 0) == tp_ref[...], 1.0, 0.0
    )
    held = jnp.sum(chosen, axis=1, keepdims=True)
    top_zero = (dot(chosen.astype(BF16), one[...]) / jnp.maximum(held, 1.0)).astype(BF16)
    top_stride = tops + PAD
    put_rows(ts, top_stride, 0, tops, dot(top_zero, tw_ref[0]).astype(BF16).astype(F32))
    put_rows(tr, top_stride, 0, tops, dot(top_zero, tw_ref[1]).astype(BF16).astype(F32))
    edge_sums(
        tops, ts_ref.shape[0], ts_ref, tr_ref, trv_ref, ts, top_stride, tr, top_stride, buf, hid, acc
    )
    top_one = updated(top_zero, acc[0:tops, :], tw_ref, g_ref[2:3, :]).astype(BF16)
    for at in range(0, count, size):
        rows = slice(at, at + size)
        lifted = dot(picks(tp_ref[:, rows], tops), top_one)
        one[rows, :] = (one[rows, :].astype(F32) + lifted).astype(BF16)
    coarse_out[...] = one[0:size, :]
    for at in range(0, fine.shape[0], ROWS):
        rows = slice(at, at + ROWS)
        lifted = dot(picks(p_ref[:, rows], count), one[...])
        fine_out[rows, :] = (fine[rows, :].astype(F32) + lifted).astype(BF16)


def call(kernel, outs, specs, scratch, *operands):
    return pl.pallas_call(
        kernel,
        out_shape=outs,
        in_specs=specs,
        out_specs=jax.tree.map(lambda _: VMEM_SPEC, outs),
        scratch_shapes=scratch,
        compiler_params=pltpu.CompilerParams(vmem_limit_bytes=VMEM_LIMIT),
    )(*operands)


def body(
    fine_nodes,
    fine_weights,
    coarse_weights,
    top_weights,
    gains,
    send_list,
    fine_sender,
    fine_receiver,
    pool_owner,
    pool_local,
    coarse_sender,
    coarse_receiver,
    top_parent,
    top_sender,
    top_receiver,
):
    nodes, width = fine_nodes.shape
    members = lax.axis_size("gx")
    me = lax.axis_index("gx")
    size = nodes // 8
    count = size * members
    tops = count // 8
    listed = send_list.shape[-1]
    edges = fine_sender.shape[-1]
    shape = jax.ShapeDtypeStruct

    halo = call(
        halo_kernel,
        [shape((listed, width), BF16)] * 4,
        [SMEM_SPEC, VMEM_SPEC],
        [
            pltpu.VMEM((2 * (nodes + PAD), LANES), F32),
            pltpu.VMEM((2 * (listed + PAD), LANES), F32),
        ],
        send_list.reshape(-1),
        fine_nodes,
    )
    arrived = [
        shifted(halo[slot], axis, distance, False)
        for slot, (axis, distance) in enumerate((("gx", 1), ("gx", -1), ("gy", 1), ("gy", -1)))
    ]

    owner = pool_owner.reshape(1, -1)
    local = pool_local.reshape(1, -1)
    ahead = lax.rem(owner - me + members, members) * size + local
    behind = lax.rem(me - owner + members, members) * size + local
    counts = call(
        functools.partial(count_kernel, members),
        shape((members, size), jnp.int32),
        [VMEM_SPEC],
        [],
        ahead,
    )
    share = jnp.concatenate(
        [coarse_sender.reshape(1, -1), coarse_receiver.reshape(1, -1), top_parent.reshape(1, -1)],
        axis=1,
    )
    mixed = [
        jnp.concatenate([share, counts[d : d + 1]], axis=1) for d in range(members)
    ]
    mixed = [mixed[0]] + [shifted(mixed[d], "gx", d, True) for d in range(1, members)]
    per = coarse_sender.shape[-1]
    senders = jnp.concatenate([piece[0, :per] for piece in mixed])
    senders = lax.rem(me - senders // size + members, members) * size + lax.rem(senders, size)
    receivers = jnp.concatenate([piece[0, per : 2 * per] + d * size for d, piece in enumerate(mixed)])
    tops_of = jnp.concatenate([piece[:, 2 * per : 2 * per + size] for piece in mixed], axis=1)
    children = jnp.concatenate([piece[:, 2 * per + size :] for piece in mixed], axis=0)

    chunk = min(CHUNK, edges)
    fine_one, *parts = call(
        functools.partial(fine_kernel, members),
        [shape((nodes, width), BF16)] + [shape((size, width), BF16)] * members,
        [SMEM_SPEC] * 2 + [VMEM_SPEC] * 9,
        [
            pltpu.VMEM((2 * (nodes + 4 * listed + PAD), LANES), F32),
            pltpu.VMEM((2 * (nodes + PAD), LANES), F32),
            pltpu.VMEM((2 * (chunk + PAD), LANES), F32),
            pltpu.VMEM((chunk, width), BF16),
            pltpu.VMEM((nodes, width), F32),
        ],
        fine_sender.reshape(-1),
        fine_receiver.reshape(-1),
        fine_receiver.reshape(-1, chunk),
        ahead,
        fine_nodes,
        *arrived,
        fine_weights,
        gains,
    )
    parts = [parts[0]] + [shifted(parts[d], "gx", d, True) for d in range(1, members)]
    zero = call(
        functools.partial(mean_kernel, members),
        shape((size, width), BF16),
        [VMEM_SPEC] * (1 + members),
        [],
        children,
        *parts,
    )
    zeros = [zero] + [shifted(zero, "gx", d, True) for d in range(1, members)]

    top_edges = top_sender.shape[-1]
    chunk = min(CHUNK, per * members, top_edges)
    fine_state, coarse_state = call(
        functools.partial(upper_kernel, members),
        [shape((nodes, width), BF16), shape((size, width), BF16)],
        [SMEM_SPEC] * 2 + [VMEM_SPEC] + [SMEM_SPEC] * 2 + [VMEM_SPEC] * (7 + members),
        [
            pltpu.VMEM((2 * (count + PAD), LANES), F32),
            pltpu.VMEM((2 * (count + PAD), LANES), F32),
            pltpu.VMEM((2 * (chunk + PAD), LANES), F32),
            pltpu.VMEM((chunk, width), BF16),
            pltpu.VMEM((count, width), F32),
            pltpu.VMEM((count, width), BF16),
            pltpu.VMEM((count, width), BF16),
        ],
        senders,
        receivers,
        receivers.reshape(-1, chunk),
        top_sender.reshape(-1),
        top_receiver.reshape(-1),
        top_receiver.reshape(-1, chunk),
        tops_of,
        behind,
        fine_one,
        coarse_weights,
        top_weights,
        gains,
        *zeros,
    )
    return (fine_state, coarse_state[None])


def solution(mesh):
    placed = (
        P(("gx", "gy"), None),
        P(),
        P(),
        P(),
        P(),
        P("gx", "gy", None, None),
        P("gx", "gy", None),
        P("gx", "gy", None),
        P(("gx", "gy"), None),
        P(("gx", "gy")),
        P("gy", "gx"),
        P("gy", "gx"),
        P("gy", "gx"),
        P("gy", None),
        P("gy", None),
    )
    return jax.shard_map(
        body,
        mesh=mesh,
        in_specs=placed,
        out_specs=(P(("gx", "gy"), None), P("gy", "gx", None)),
        check_vma=False,
    )
```

```python
import functools
import math

import jax
import jax.numpy as jnp
from jax import lax
from jax.experimental import pallas as pl
from jax.experimental.pallas import tpu as pltpu
from jax.sharding import PartitionSpec as P

F32 = jnp.float32
BF16 = jnp.bfloat16
LANES = 128
TAIL = 16
PAD = 8
FINE_CHUNK = 512
COARSE_CHUNK = 512
ROWS = 2048
LIFT = 256
VMEM_SPARE = 12 << 20

SMEM_SPEC = pl.BlockSpec(memory_space=pltpu.SMEM)
VMEM_SPEC = pl.BlockSpec(memory_space=pltpu.VMEM)
LOOSE_SPEC = pl.BlockSpec(memory_space=pltpu.VMEM)
HBM_SPEC = pl.BlockSpec(memory_space=pl.ANY)


def shifted(block, axis, distance, wrap):
    count = lax.axis_size(axis)
    route = []
    for i in range(count):
        j = i + distance
        if wrap:
            route.append((i, j % count))
        elif 0 <= j < count:
            route.append((i, j))
    return lax.ppermute(block, axis, route)


def dot(a, b):
    return jnp.dot(a, b, preferred_element_type=F32)


def silu(v):
    return (0.5 * v) * (1.0 + jnp.tanh(0.5 * v))


def put_rows(table, stride, begin, rows, values):
    table[begin : begin + rows, :] = values[:, :LANES]
    table[stride + begin : stride + begin + rows, :] = values[:, LANES:]


def project_into(table, stride, begin, states, weight):
    rows = states.shape[0]
    step = min(rows, 512)
    for at in range(0, rows, step):
        term = dot(states[at : at + step, :], weight).astype(BF16).astype(F32)
        put_rows(table, stride, begin + at, step, term)


def selection(indices, begin, rows):
    columns = indices.shape[1]
    number = lax.broadcasted_iota(jnp.int32, (rows, columns), 0) + begin
    return jnp.where(number == indices, 1.0, 0.0).astype(BF16)


def gather_rows(base, begin, end, s_ref, r_ref, ts, s_stride, tr, r_stride, buf, buf_stride):
    lines = 4
    length = (end - begin) // lines
    starts = [pl.multiple_of(base + begin + line * length, length) for line in range(lines)]
    s_of = [s_ref.at[:, pl.ds(start, length)] for start in starts]
    r_of = [r_ref.at[:, pl.ds(start, length)] for start in starts]
    for j in range(length):
        for line in range(lines):
            s = s_of[line][0, j]
            r = r_of[line][0, j]
            buf[pl.ds(begin + line * length + j, 2, stride=buf_stride), :] = (
                ts[pl.ds(s, 2, stride=s_stride), :] + tr[pl.ds(r, 2, stride=r_stride), :]
            )


def edge_sums(nodes, chunk, s_ref, r_ref, rv_ref, ts, s_stride, tr, r_stride, buf, hid, acc):
    turns = s_ref.shape[1] // chunk
    block = min(ROWS, nodes)
    stride = buf.shape[0] // 2
    acc[0:nodes, :] = jnp.zeros((nodes, 2 * LANES), F32)

    def gather(c):
        gather_rows(c * chunk, 0, chunk, s_ref, r_ref, ts, s_stride, tr, r_stride, buf, stride)

    def activate(slot):
        hid[slot, 0:chunk, :LANES] = silu(buf[0:chunk, :]).astype(BF16)
        hid[slot, 0:chunk, LANES:] = silu(buf[stride : stride + chunk, :]).astype(BF16)

    def sums(c, at):
        targets = rv_ref[:, pl.ds(pl.multiple_of(c * chunk, chunk), chunk)]
        return dot(selection(targets, at, block), hid[lax.rem(c, 2), 0:chunk, :])

    gather(0)
    activate(0)

    def turn(c, carry):
        for at in range(0, nodes - block, block):
            acc[at : at + block, :] += sums(c, at)
        added = sums(c, nodes - block)
        gather(c + 1)
        acc[nodes - block : nodes, :] += added
        activate(lax.rem(c + 1, 2))
        return carry

    if turns > 1:
        lax.fori_loop(0, turns - 1, turn, 0)
    for at in range(0, nodes, block):
        acc[at : at + block, :] += sums(turns - 1, at)


def updated(states, summed, w_ref, gain):
    aggregate = dot(summed.astype(BF16), w_ref[2]).astype(BF16)
    inner = silu(dot(states, w_ref[3]) + dot(aggregate, w_ref[4])).astype(BF16)
    output = dot(inner, w_ref[5])
    centred = output - jnp.mean(output, axis=1, keepdims=True)
    spread = jnp.mean(centred * centred, axis=1, keepdims=True)
    return states.astype(F32) + gain * centred * lax.rsqrt(spread + 1e-05)


def halo_kernel(l_ref, nodes, *refs):
    outs, (table, buf) = refs[:4], refs[4:]
    rows = nodes.shape[0]
    listed = outs[0].shape[0]
    unroll = 128
    lines = 4
    put_rows(table, rows + PAD, 0, rows, nodes[...].astype(F32))
    for d in range(4):

        def some(c, carry):
            base = pl.multiple_of(c * unroll, unroll)
            length = unroll // lines
            of = [l_ref.at[:, pl.ds(base + line * length, length)] for line in range(lines)]
            for j in range(length):
                for line in range(lines):
                    i = of[line][d, j]
                    buf[pl.ds(base + line * length + j, 2, stride=listed + PAD), :] = table[
                        pl.ds(i, 2, stride=rows + PAD), :
                    ]
            return carry

        lax.fori_loop(0, listed // unroll, some, 0)
        outs[d][:, :LANES] = buf[0:listed, :].astype(BF16)
        outs[d][:, LANES:] = buf[listed + PAD : 2 * listed + PAD, :].astype(BF16)


def count_kernel(members, p_ref, out):
    size = out.shape[1]
    eye = lax.broadcasted_iota(jnp.int32, (size, size), 0) == lax.broadcasted_iota(
        jnp.int32, (size, size), 1
    )
    parents = p_ref[...]
    line = lax.broadcasted_iota(jnp.int32, (TAIL, size), 0)
    for d in range(members):
        chosen = jnp.where(
            lax.broadcasted_iota(jnp.int32, (size, parents.shape[1]), 0) + d * size == parents,
            1.0,
            0.0,
        )
        column = jnp.sum(chosen, axis=1, keepdims=True)
        row = jnp.sum(jnp.where(eye, column, 0.0), axis=0, keepdims=True)
        upper = jnp.floor(row * (1.0 / 256.0))
        lower = row - upper * 256.0
        out[d * TAIL : (d + 1) * TAIL, :] = jnp.where(
            line == 0, lower, jnp.where(line == 1, upper, 0.0)
        ).astype(BF16)


def started(*copies):
    for copy in copies:
        copy.start()
    return copies


def fine_kernel(members, chunk, s_hbm, r_hbm, w_hbm, rv_ref, p_ref, c_ref, nodes, h0, h1, h2, h3, g_ref, *refs):
    one, parts = refs[0], refs[1 : 1 + members]
    ts, tr, buf, hid, acc, s_ref, r_ref, w_ref, sems = refs[1 + members :]
    early, late, senders, receivers = started(
        pltpu.make_async_copy(w_hbm.at[0:2], w_ref.at[0:2], sems.at[0]),
        pltpu.make_async_copy(w_hbm.at[2:6], w_ref.at[2:6], sems.at[1]),
        pltpu.make_async_copy(s_hbm, s_ref, sems.at[2]),
        pltpu.make_async_copy(r_hbm, r_ref, sems.at[3]),
    )
    count = nodes.shape[0]
    listed = h0.shape[0]
    s_stride = count + 4 * listed + PAD
    r_stride = count + PAD
    put_rows(tr, r_stride, count, PAD, jnp.zeros((PAD, 2 * LANES), F32))
    early.wait()
    project_into(ts, s_stride, 0, nodes, w_ref[0])
    for d, halo in enumerate((h0, h1, h2, h3)):
        project_into(ts, s_stride, count + d * listed, halo, w_ref[0])
    project_into(tr, r_stride, 0, nodes, w_ref[1])
    senders.wait()
    receivers.wait()
    edge_sums(count, chunk, s_ref, r_ref, rv_ref, ts, s_stride, tr, r_stride, buf, hid, acc)
    late.wait()
    gain = g_ref[0:1, :]
    step = 512
    for at in range(0, count, step):
        rows = slice(at, at + step)
        one[rows, :] = updated(nodes[rows, :], acc[rows, :], w_ref, gain).astype(BF16)
    parents = p_ref[...]
    size = parts[0].shape[0] - TAIL
    for d in range(members):
        parts[d][0:size, :] = dot(selection(parents, d * size, size), one[...]).astype(BF16)
        parts[d][size : size + TAIL, :] = c_ref[d * TAIL : (d + 1) * TAIL, :]


def mean_kernel(members, *refs):
    pieces, out = refs[:members], refs[members]
    size = out.shape[0]
    eye = lax.broadcasted_iota(jnp.int32, (size, size), 0) == lax.broadcasted_iota(
        jnp.int32, (size, size), 1
    )
    total = pieces[0][...].astype(F32)
    for piece in pieces[1:]:
        total = total + piece[...].astype(F32)
    children = total[size : size + 1, :] + 256.0 * total[size + 1 : size + 2, :]
    column = jnp.sum(jnp.where(eye, children, 0.0), axis=1, keepdims=True)
    out[...] = (total[0:size, :] / jnp.maximum(column, 1.0)).astype(BF16)


def turned(row):
    n = row.shape[1]
    return jnp.concatenate(
        [
            jnp.transpose(jnp.broadcast_to(row[:, at : at + LANES], (LANES, LANES)))
            for at in range(0, n, LANES)
        ],
        axis=0,
    )


def picks(row, columns):
    column = turned(row)
    lane = lax.broadcasted_iota(jnp.int32, column.shape, 1)
    return jnp.concatenate(
        [
            jnp.where(column == lane + at, 1.0, 0.0).astype(BF16)
            for at in range(0, columns, LANES)
        ],
        axis=1,
    )


def upper_kernel(
    members,
    chunk,
    cs_hbm,
    cr_hbm,
    ts_hbm,
    tr_hbm,
    cw_hbm,
    tw_hbm,
    crv_ref,
    trv_ref,
    tp_ref,
    p_ref,
    fine,
    g_ref,
    *refs,
):
    pieces = refs[:members]
    fine_out, coarse_out = refs[members : members + 2]
    (
        ts,
        tr,
        buf,
        hid,
        acc,
        zero,
        one,
        last,
        cs_ref,
        cr_ref,
        es_ref,
        er_ref,
        cw_ref,
        tw_ref,
        sems,
    ) = refs[members + 2 :]
    copies = started(
        pltpu.make_async_copy(cw_hbm, cw_ref, sems.at[0]),
        pltpu.make_async_copy(cs_hbm, cs_ref, sems.at[1]),
        pltpu.make_async_copy(cr_hbm, cr_ref, sems.at[2]),
        pltpu.make_async_copy(ts_hbm, es_ref, sems.at[3]),
        pltpu.make_async_copy(tr_hbm, er_ref, sems.at[4]),
        pltpu.make_async_copy(tw_hbm, tw_ref, sems.at[5]),
    )
    size = pieces[0].shape[0]
    count = size * members
    tops = count // 8
    stride = count + PAD
    for d in range(members):
        zero[d * size : (d + 1) * size, :] = pieces[d][...]
    copies[0].wait()
    project_into(ts, stride, 0, zero, cw_ref[0])
    project_into(tr, stride, 0, zero, cw_ref[1])
    for copy in copies[1:]:
        copy.wait()
    edge_sums(count, chunk, cs_ref, cr_ref, crv_ref, ts, stride, tr, stride, buf, hid, acc)
    gain = g_ref[1:2, :]
    step = min(count, 512)
    for at in range(0, count, step):
        rows = slice(at, at + step)
        one[rows, :] = updated(zero[rows, :], acc[rows, :], cw_ref, gain).astype(BF16)
    chosen = jnp.where(
        lax.broadcasted_iota(jnp.int32, (tops, count), 0) == tp_ref[...], 1.0, 0.0
    )
    held = jnp.sum(chosen, axis=1, keepdims=True)
    top_zero = (dot(chosen.astype(BF16), one[...]) / jnp.maximum(held, 1.0)).astype(BF16)
    top_stride = tops + PAD
    put_rows(ts, top_stride, 0, tops, dot(top_zero, tw_ref[0]).astype(BF16).astype(F32))
    put_rows(tr, top_stride, 0, tops, dot(top_zero, tw_ref[1]).astype(BF16).astype(F32))
    edge_sums(tops, chunk, es_ref, er_ref, trv_ref, ts, top_stride, tr, top_stride, buf, hid, acc)
    top_one = updated(top_zero, acc[0:tops, :], tw_ref, g_ref[2:3, :]).astype(BF16)
    for at in range(0, count, size):
        rows = slice(at, at + size)
        lifted = dot(picks(tp_ref[:, rows], tops), top_one)
        one[rows, :] = (one[rows, :].astype(F32) + lifted).astype(BF16)
    (done,) = started(pltpu.make_async_copy(one.at[0:size, :], coarse_out, sems.at[0]))
    leaving = [done]
    step = fine.shape[0] // 4
    for k in range(4):
        for at in range(k * step, (k + 1) * step, LIFT):
            rows = slice(at, at + LIFT)
            lifted = dot(picks(p_ref[:, rows], count), one[...])
            last[rows, :] = (fine[rows, :].astype(F32) + lifted).astype(BF16)
        rows = pl.ds(k * step, step)
        leaving += started(
            pltpu.make_async_copy(last.at[rows, :], fine_out.at[rows, :], sems.at[1 + k])
        )
    for copy in leaving:
        copy.wait()


def call(kernel, outs, out_spec, specs, scratch, *operands):
    held = sum(
        math.prod(s.shape) * s.dtype.itemsize for s in scratch if s.memory_space == pltpu.VMEM
    )
    operands = [
        pltpu.with_memory_space_constraint(x, pltpu.VMEM) if spec is VMEM_SPEC else x
        for x, spec in zip(operands, specs)
    ]
    return pl.pallas_call(
        kernel,
        out_shape=outs,
        in_specs=specs,
        out_specs=[out_spec for _ in outs],
        scratch_shapes=scratch,
        compiler_params=pltpu.CompilerParams(vmem_limit_bytes=held + VMEM_SPARE),
    )(*operands)


def body(
    fine_nodes,
    fine_weights,
    coarse_weights,
    top_weights,
    gains,
    send_list,
    fine_sender,
    fine_receiver,
    pool_owner,
    pool_local,
    coarse_sender,
    coarse_receiver,
    top_parent,
    top_sender,
    top_receiver,
):
    nodes, width = fine_nodes.shape
    members = lax.axis_size("gx")
    me = lax.axis_index("gx")
    size = nodes // 8
    count = size * members
    tops = count // 8
    listed = send_list.shape[-1]
    edges = fine_sender.shape[-1]
    shape = jax.ShapeDtypeStruct

    halo = list(
        call(
            halo_kernel,
            [shape((listed, width), BF16)] * 4,
            LOOSE_SPEC,
            [SMEM_SPEC, LOOSE_SPEC],
            [
                pltpu.VMEM((2 * (nodes + PAD), LANES), F32),
                pltpu.VMEM((2 * (listed + PAD), LANES), F32),
            ],
            send_list.reshape(4, listed),
            fine_nodes,
        )
    )
    halo[0], pool_owner, pool_local = lax.optimization_barrier((halo[0], pool_owner, pool_local))
    arrived = [
        shifted(halo[slot], axis, distance, False)
        for slot, (axis, distance) in enumerate((("gx", 1), ("gx", -1), ("gy", 1), ("gy", -1)))
    ]
    owner = pool_owner.reshape(1, -1)
    local = pool_local.reshape(1, -1)
    ahead = lax.rem(owner - me + members, members) * size + local
    behind = lax.rem(me - owner + members, members) * size + local
    (counts,) = call(
        functools.partial(count_kernel, members),
        [shape((members * TAIL, size), BF16)],
        LOOSE_SPEC,
        [LOOSE_SPEC],
        [],
        ahead,
    )
    chunk = min(FINE_CHUNK, edges)
    fine_sender = fine_sender.reshape(1, edges)
    fine_receiver = fine_receiver.reshape(1, edges)
    fine_one, *parts = call(
        functools.partial(fine_kernel, members, chunk),
        [shape((nodes, width), BF16)] + [shape((size + TAIL, width), BF16)] * members,
        LOOSE_SPEC,
        [HBM_SPEC] * 3 + [LOOSE_SPEC] * 3 + [VMEM_SPEC] * 5 + [LOOSE_SPEC],
        [
            pltpu.VMEM((2 * (nodes + 4 * listed + PAD), LANES), F32),
            pltpu.VMEM((2 * (nodes + PAD), LANES), F32),
            pltpu.VMEM((2 * (chunk + PAD), LANES), F32),
            pltpu.VMEM((2, chunk, width), BF16),
            pltpu.VMEM((nodes, width), F32),
            pltpu.SMEM((1, edges), jnp.int32),
            pltpu.SMEM((1, edges), jnp.int32),
            pltpu.VMEM(fine_weights.shape, BF16),
            pltpu.SemaphoreType.DMA((4,)),
        ],
        fine_sender,
        fine_receiver,
        fine_weights,
        fine_receiver,
        ahead,
        counts,
        fine_nodes,
        *arrived,
        gains,
    )
    parts = [parts[0]] + [shifted(parts[d], "gx", d, True) for d in range(1, members)]
    if members > 1:
        parts[1], coarse_sender, coarse_receiver, top_parent = lax.optimization_barrier(
            (parts[1], coarse_sender, coarse_receiver, top_parent)
        )
    share = jnp.concatenate(
        [coarse_sender.reshape(1, -1), coarse_receiver.reshape(1, -1), top_parent.reshape(1, -1)],
        axis=1,
    )
    mixed = [share] + [shifted(share, "gx", d, True) for d in range(1, members)]
    per = coarse_sender.shape[-1]
    senders = jnp.concatenate([piece[:, :per] for piece in mixed], axis=1)
    senders = lax.rem(me - senders // size + members, members) * size + lax.rem(senders, size)
    receivers = jnp.concatenate(
        [piece[:, per : 2 * per] + d * size for d, piece in enumerate(mixed)], axis=1
    )
    tops_of = jnp.concatenate([piece[:, 2 * per :] for piece in mixed], axis=1)

    (zero,) = call(
        functools.partial(mean_kernel, members),
        [shape((size, width), BF16)],
        LOOSE_SPEC,
        [LOOSE_SPEC] + [VMEM_SPEC] * (members - 1),
        [],
        *parts,
    )
    zeros = [zero] + [shifted(zero, "gx", d, True) for d in range(1, members)]

    top_edges = top_sender.shape[-1]
    chunk = min(COARSE_CHUNK, per * members, top_edges)
    fine_state, coarse_state = call(
        functools.partial(upper_kernel, members, chunk),
        [shape((nodes, width), BF16), shape((size, width), BF16)],
        HBM_SPEC,
        [HBM_SPEC] * 6 + [LOOSE_SPEC] * 4 + [VMEM_SPEC] + [LOOSE_SPEC] * 2 + [VMEM_SPEC] * (members - 1),
        [
            pltpu.VMEM((2 * (count + PAD), LANES), F32),
            pltpu.VMEM((2 * (count + PAD), LANES), F32),
            pltpu.VMEM((2 * (chunk + PAD), LANES), F32),
            pltpu.VMEM((2, chunk, width), BF16),
            pltpu.VMEM((count, width), F32),
            pltpu.VMEM((count, width), BF16),
            pltpu.VMEM((count, width), BF16),
            pltpu.VMEM((nodes, width), BF16),
            pltpu.SMEM((1, per * members), jnp.int32),
            pltpu.SMEM((1, per * members), jnp.int32),
            pltpu.SMEM((1, top_edges), jnp.int32),
            pltpu.SMEM((1, top_edges), jnp.int32),
            pltpu.VMEM(coarse_weights.shape, BF16),
            pltpu.VMEM(top_weights.shape, BF16),
            pltpu.SemaphoreType.DMA((6,)),
        ],
        senders,
        receivers,
        top_sender,
        top_receiver,
        coarse_weights,
        top_weights,
        receivers,
        top_receiver,
        tops_of,
        behind,
        fine_one,
        gains,
        *zeros,
    )
    return (fine_state, coarse_state[None])


def solution(mesh):
    placed = (
        P(("gx", "gy"), None),
        P(),
        P(),
        P(),
        P(),
        P("gx", "gy", None, None),
        P("gx", "gy", None),
        P("gx", "gy", None),
        P(("gx", "gy"), None),
        P(("gx", "gy")),
        P("gy", "gx"),
        P("gy", "gx"),
        P("gy", "gx"),
        P("gy", None),
        P("gy", None),
    )
    return jax.shard_map(
        body,
        mesh=mesh,
        in_specs=placed,
        out_specs=(P(("gx", "gy"), None), P("gy", "gx", None)),
        check_vma=False,
    )
```

```python
import functools
import math

import jax
import jax.numpy as jnp
from jax import lax
from jax.experimental import pallas as pl
from jax.experimental.pallas import tpu as pltpu
from jax.sharding import PartitionSpec as P

F32 = jnp.float32
BF16 = jnp.bfloat16
LANES = 128
TAIL = 16
PAD = 8
FINE_CHUNK = 1024
COARSE_CHUNK = 512
ROWS = 2048
LIFT = 256
VMEM_SPARE = 12 << 20

SMEM_SPEC = pl.BlockSpec(memory_space=pltpu.SMEM)
VMEM_SPEC = pl.BlockSpec(memory_space=pltpu.VMEM)
LOOSE_SPEC = pl.BlockSpec(memory_space=pltpu.VMEM)
HBM_SPEC = pl.BlockSpec(memory_space=pl.ANY)


def shifted(block, axis, distance, wrap):
    count = lax.axis_size(axis)
    route = []
    for i in range(count):
        j = i + distance
        if wrap:
            route.append((i, j % count))
        elif 0 <= j < count:
            route.append((i, j))
    return lax.ppermute(block, axis, route)


def dot(a, b):
    return jnp.dot(a, b, preferred_element_type=F32)


def silu(v):
    return (0.5 * v) * (1.0 + jnp.tanh(0.5 * v))


def put_rows(table, stride, begin, rows, values):
    table[begin : begin + rows, :] = values[:, :LANES]
    table[stride + begin : stride + begin + rows, :] = values[:, LANES:]


def project_into(table, stride, begin, states, weight):
    rows = states.shape[0]
    step = min(rows, 512)
    for at in range(0, rows, step):
        term = dot(states[at : at + step, :], weight).astype(BF16).astype(F32)
        put_rows(table, stride, begin + at, step, term)


def selection(indices, begin, rows):
    columns = indices.shape[1]
    number = lax.broadcasted_iota(jnp.int32, (rows, columns), 0) + begin
    return jnp.where(number == indices, 1.0, 0.0).astype(BF16)


def gather_rows(base, begin, end, s_ref, r_ref, ts, s_stride, tr, r_stride, buf, buf_stride):
    lines = 4
    length = (end - begin) // lines
    starts = [pl.multiple_of(base + begin + line * length, length) for line in range(lines)]
    s_of = [s_ref.at[:, pl.ds(start, length)] for start in starts]
    r_of = [r_ref.at[:, pl.ds(start, length)] for start in starts]
    for j in range(length):
        for line in range(lines):
            s = s_of[line][0, j]
            r = r_of[line][0, j]
            buf[pl.ds(begin + line * length + j, 2, stride=buf_stride), :] = (
                ts[pl.ds(s, 2, stride=s_stride), :] + tr[pl.ds(r, 2, stride=r_stride), :]
            )


def edge_sums(nodes, chunk, s_ref, r_ref, rv_ref, ts, s_stride, tr, r_stride, buf, hid, acc):
    turns = s_ref.shape[1] // chunk
    block = min(ROWS, nodes)
    stride = buf.shape[0] // 2
    acc[0:nodes, :] = jnp.zeros((nodes, 2 * LANES), F32)

    def gather(c):
        gather_rows(c * chunk, 0, chunk, s_ref, r_ref, ts, s_stride, tr, r_stride, buf, stride)

    def activate(slot):
        hid[slot, 0:chunk, :LANES] = silu(buf[0:chunk, :]).astype(BF16)
        hid[slot, 0:chunk, LANES:] = silu(buf[stride : stride + chunk, :]).astype(BF16)

    def sums(c, at):
        targets = rv_ref[:, pl.ds(pl.multiple_of(c * chunk, chunk), chunk)]
        return dot(selection(targets, at, block), hid[lax.rem(c, 2), 0:chunk, :])

    gather(0)
    activate(0)

    def turn(c, carry):
        for at in range(0, nodes - block, block):
            acc[at : at + block, :] += sums(c, at)
        added = sums(c, nodes - block)
        gather(c + 1)
        acc[nodes - block : nodes, :] += added
        activate(lax.rem(c + 1, 2))
        return carry

    if turns > 1:
        lax.fori_loop(0, turns - 1, turn, 0)
    for at in range(0, nodes, block):
        acc[at : at + block, :] += sums(turns - 1, at)


def updated(states, summed, w_ref, gain):
    aggregate = dot(summed.astype(BF16), w_ref[2]).astype(BF16)
    inner = silu(dot(states, w_ref[3]) + dot(aggregate, w_ref[4])).astype(BF16)
    output = dot(inner, w_ref[5])
    centred = output - jnp.mean(output, axis=1, keepdims=True)
    spread = jnp.mean(centred * centred, axis=1, keepdims=True)
    return states.astype(F32) + gain * centred * lax.rsqrt(spread + 1e-05)


def halo_kernel(l_ref, nodes, *refs):
    outs, (table, buf) = refs[:4], refs[4:]
    rows = nodes.shape[0]
    listed = outs[0].shape[0]
    unroll = 128
    lines = 4
    put_rows(table, rows + PAD, 0, rows, nodes[...].astype(F32))
    for d in range(4):

        def some(c, carry):
            base = pl.multiple_of(c * unroll, unroll)
            length = unroll // lines
            of = [l_ref.at[:, pl.ds(base + line * length, length)] for line in range(lines)]
            for j in range(length):
                for line in range(lines):
                    i = of[line][d, j]
                    buf[pl.ds(base + line * length + j, 2, stride=listed + PAD), :] = table[
                        pl.ds(i, 2, stride=rows + PAD), :
                    ]
            return carry

        lax.fori_loop(0, listed // unroll, some, 0)
        outs[d][:, :LANES] = buf[0:listed, :].astype(BF16)
        outs[d][:, LANES:] = buf[listed + PAD : 2 * listed + PAD, :].astype(BF16)


def started(*copies):
    for copy in copies:
        copy.start()
    return copies


def count_kernel(members, p_ref, w_hbm, s_hbm, r_hbm, out, w_out, s_out, r_out, sems):
    copies = started(
        pltpu.make_async_copy(w_hbm, w_out, sems.at[0]),
        pltpu.make_async_copy(s_hbm, s_out, sems.at[1]),
        pltpu.make_async_copy(r_hbm, r_out, sems.at[2]),
    )
    size = out.shape[1]
    eye = lax.broadcasted_iota(jnp.int32, (size, size), 0) == lax.broadcasted_iota(
        jnp.int32, (size, size), 1
    )
    parents = p_ref[...]
    line = lax.broadcasted_iota(jnp.int32, (TAIL, size), 0)
    for d in range(members):
        chosen = jnp.where(
            lax.broadcasted_iota(jnp.int32, (size, parents.shape[1]), 0) + d * size == parents,
            1.0,
            0.0,
        )
        column = jnp.sum(chosen, axis=1, keepdims=True)
        row = jnp.sum(jnp.where(eye, column, 0.0), axis=0, keepdims=True)
        upper = jnp.floor(row * (1.0 / 256.0))
        lower = row - upper * 256.0
        out[d * TAIL : (d + 1) * TAIL, :] = jnp.where(
            line == 0, lower, jnp.where(line == 1, upper, 0.0)
        ).astype(BF16)
    for copy in copies:
        copy.wait()


def fine_kernel(members, chunk, s_hbm, r_hbm, w_ref, rv_ref, p_ref, c_ref, nodes, h0, h1, h2, h3, g_ref, *refs):
    one, parts = refs[0], refs[1 : 1 + members]
    ts, tr, buf, hid, acc, s_ref, r_ref, sems = refs[1 + members :]
    senders, receivers = started(
        pltpu.make_async_copy(s_hbm, s_ref, sems.at[0]),
        pltpu.make_async_copy(r_hbm, r_ref, sems.at[1]),
    )
    count = nodes.shape[0]
    listed = h0.shape[0]
    s_stride = count + 4 * listed + PAD
    r_stride = count + PAD
    put_rows(tr, r_stride, count, PAD, jnp.zeros((PAD, 2 * LANES), F32))
    project_into(ts, s_stride, 0, nodes, w_ref[0])
    for d, halo in enumerate((h0, h1, h2, h3)):
        project_into(ts, s_stride, count + d * listed, halo, w_ref[0])
    project_into(tr, r_stride, 0, nodes, w_ref[1])
    senders.wait()
    receivers.wait()
    edge_sums(count, chunk, s_ref, r_ref, rv_ref, ts, s_stride, tr, r_stride, buf, hid, acc)
    gain = g_ref[0:1, :]
    step = 512
    for at in range(0, count, step):
        rows = slice(at, at + step)
        one[rows, :] = updated(nodes[rows, :], acc[rows, :], w_ref, gain).astype(BF16)
    parents = p_ref[...]
    size = parts[0].shape[0] - TAIL
    for d in range(members):
        parts[d][0:size, :] = dot(selection(parents, d * size, size), one[...]).astype(BF16)
        parts[d][size : size + TAIL, :] = c_ref[d * TAIL : (d + 1) * TAIL, :]


def mean_kernel(members, *refs):
    pieces, out = refs[:members], refs[members]
    size = out.shape[0]
    eye = lax.broadcasted_iota(jnp.int32, (size, size), 0) == lax.broadcasted_iota(
        jnp.int32, (size, size), 1
    )
    total = pieces[0][...].astype(F32)
    for piece in pieces[1:]:
        total = total + piece[...].astype(F32)
    children = total[size : size + 1, :] + 256.0 * total[size + 1 : size + 2, :]
    column = jnp.sum(jnp.where(eye, children, 0.0), axis=1, keepdims=True)
    out[...] = (total[0:size, :] / jnp.maximum(column, 1.0)).astype(BF16)


def turned(row):
    n = row.shape[1]
    return jnp.concatenate(
        [
            jnp.transpose(jnp.broadcast_to(row[:, at : at + LANES], (LANES, LANES)))
            for at in range(0, n, LANES)
        ],
        axis=0,
    )


def picks(row, columns):
    column = turned(row)
    lane = lax.broadcasted_iota(jnp.int32, column.shape, 1)
    return jnp.concatenate(
        [
            jnp.where(column == lane + at, 1.0, 0.0).astype(BF16)
            for at in range(0, columns, LANES)
        ],
        axis=1,
    )


def upper_kernel(
    members,
    chunk,
    cs_hbm,
    cr_hbm,
    ts_hbm,
    tr_hbm,
    cw_hbm,
    tw_hbm,
    crv_ref,
    trv_ref,
    tp_ref,
    p_ref,
    fine,
    g_ref,
    *refs,
):
    pieces = refs[:members]
    fine_out, coarse_out = refs[members : members + 2]
    (
        ts,
        tr,
        buf,
        hid,
        acc,
        zero,
        one,
        last,
        cs_ref,
        cr_ref,
        es_ref,
        er_ref,
        cw_ref,
        tw_ref,
        sems,
    ) = refs[members + 2 :]
    copies = started(
        pltpu.make_async_copy(cw_hbm, cw_ref, sems.at[0]),
        pltpu.make_async_copy(cs_hbm, cs_ref, sems.at[1]),
        pltpu.make_async_copy(cr_hbm, cr_ref, sems.at[2]),
        pltpu.make_async_copy(ts_hbm, es_ref, sems.at[3]),
        pltpu.make_async_copy(tr_hbm, er_ref, sems.at[4]),
        pltpu.make_async_copy(tw_hbm, tw_ref, sems.at[5]),
    )
    size = pieces[0].shape[0]
    count = size * members
    tops = count // 8
    stride = count + PAD
    for d in range(members):
        zero[d * size : (d + 1) * size, :] = pieces[d][...]
    copies[0].wait()
    project_into(ts, stride, 0, zero, cw_ref[0])
    project_into(tr, stride, 0, zero, cw_ref[1])
    for copy in copies[1:]:
        copy.wait()
    edge_sums(count, chunk, cs_ref, cr_ref, crv_ref, ts, stride, tr, stride, buf, hid, acc)
    gain = g_ref[1:2, :]
    step = min(count, 512)
    for at in range(0, count, step):
        rows = slice(at, at + step)
        one[rows, :] = updated(zero[rows, :], acc[rows, :], cw_ref, gain).astype(BF16)
    chosen = jnp.where(
        lax.broadcasted_iota(jnp.int32, (tops, count), 0) == tp_ref[...], 1.0, 0.0
    )
    held = jnp.sum(chosen, axis=1, keepdims=True)
    top_zero = (dot(chosen.astype(BF16), one[...]) / jnp.maximum(held, 1.0)).astype(BF16)
    top_stride = tops + PAD
    put_rows(ts, top_stride, 0, tops, dot(top_zero, tw_ref[0]).astype(BF16).astype(F32))
    put_rows(tr, top_stride, 0, tops, dot(top_zero, tw_ref[1]).astype(BF16).astype(F32))
    edge_sums(tops, chunk, es_ref, er_ref, trv_ref, ts, top_stride, tr, top_stride, buf, hid, acc)
    top_one = updated(top_zero, acc[0:tops, :], tw_ref, g_ref[2:3, :]).astype(BF16)
    for at in range(0, count, size):
        rows = slice(at, at + size)
        lifted = dot(picks(tp_ref[:, rows], tops), top_one)
        one[rows, :] = (one[rows, :].astype(F32) + lifted).astype(BF16)
    (done,) = started(pltpu.make_async_copy(one.at[0:size, :], coarse_out, sems.at[0]))
    leaving = [done]
    step = fine.shape[0] // 4
    for k in range(4):
        for at in range(k * step, (k + 1) * step, LIFT):
            rows = slice(at, at + LIFT)
            lifted = dot(picks(p_ref[:, rows], count), one[...])
            last[rows, :] = (fine[rows, :].astype(F32) + lifted).astype(BF16)
        rows = pl.ds(k * step, step)
        leaving += started(
            pltpu.make_async_copy(last.at[rows, :], fine_out.at[rows, :], sems.at[1 + k])
        )
    for copy in leaving:
        copy.wait()


def call(kernel, outs, out_spec, specs, scratch, *operands):
    held = sum(
        math.prod(s.shape) * s.dtype.itemsize for s in scratch if getattr(s, "memory_space", None) == pltpu.VMEM
    )
    operands = [
        pltpu.with_memory_space_constraint(x, pltpu.VMEM) if spec is VMEM_SPEC else x
        for x, spec in zip(operands, specs)
    ]
    return pl.pallas_call(
        kernel,
        out_shape=outs,
        in_specs=specs,
        out_specs=[out_spec for _ in outs],
        scratch_shapes=scratch,
        compiler_params=pltpu.CompilerParams(vmem_limit_bytes=held + VMEM_SPARE),
    )(*operands)


def body(
    fine_nodes,
    fine_weights,
    coarse_weights,
    top_weights,
    gains,
    send_list,
    fine_sender,
    fine_receiver,
    pool_owner,
    pool_local,
    coarse_sender,
    coarse_receiver,
    top_parent,
    top_sender,
    top_receiver,
):
    nodes, width = fine_nodes.shape
    members = lax.axis_size("gx")
    me = lax.axis_index("gx")
    size = nodes // 8
    count = size * members
    tops = count // 8
    listed = send_list.shape[-1]
    edges = fine_sender.shape[-1]
    shape = jax.ShapeDtypeStruct

    halo = list(
        call(
            halo_kernel,
            [shape((listed, width), BF16)] * 4,
            LOOSE_SPEC,
            [SMEM_SPEC, LOOSE_SPEC],
            [
                pltpu.VMEM((2 * (nodes + PAD), LANES), F32),
                pltpu.VMEM((2 * (listed + PAD), LANES), F32),
            ],
            send_list.reshape(4, listed),
            fine_nodes,
        )
    )
    halo[0], pool_owner, pool_local = lax.optimization_barrier((halo[0], pool_owner, pool_local))
    arrived = [
        shifted(halo[slot], axis, distance, False)
        for slot, (axis, distance) in enumerate((("gx", 1), ("gx", -1), ("gy", 1), ("gy", -1)))
    ]
    owner = pool_owner.reshape(1, -1)
    local = pool_local.reshape(1, -1)
    ahead = lax.rem(owner - me + members, members) * size + local
    behind = lax.rem(me - owner + members, members) * size + local
    top_edges = top_sender.shape[-1]
    counts, fine_weights, top_sender, top_receiver = call(
        functools.partial(count_kernel, members),
        [
            shape((members * TAIL, size), BF16),
            shape(fine_weights.shape, BF16),
            shape((1, top_edges), jnp.int32),
            shape((1, top_edges), jnp.int32),
        ],
        LOOSE_SPEC,
        [LOOSE_SPEC] + [HBM_SPEC] * 3,
        [pltpu.SemaphoreType.DMA((3,))],
        ahead,
        fine_weights,
        top_sender,
        top_receiver,
    )
    chunk = min(FINE_CHUNK, edges)
    fine_sender = fine_sender.reshape(1, edges)
    fine_receiver = fine_receiver.reshape(1, edges)
    fine_one, *parts = call(
        functools.partial(fine_kernel, members, chunk),
        [shape((nodes, width), BF16)] + [shape((size + TAIL, width), BF16)] * members,
        LOOSE_SPEC,
        [HBM_SPEC] * 2 + [VMEM_SPEC] + [LOOSE_SPEC] * 3 + [VMEM_SPEC] * 5 + [LOOSE_SPEC],
        [
            pltpu.VMEM((2 * (nodes + 4 * listed + PAD), LANES), F32),
            pltpu.VMEM((2 * (nodes + PAD), LANES), F32),
            pltpu.VMEM((2 * (chunk + PAD), LANES), F32),
            pltpu.VMEM((2, chunk, width), BF16),
            pltpu.VMEM((nodes, width), F32),
            pltpu.SMEM((1, edges), jnp.int32),
            pltpu.SMEM((1, edges), jnp.int32),
            pltpu.SemaphoreType.DMA((2,)),
        ],
        fine_sender,
        fine_receiver,
        fine_weights,
        fine_receiver,
        ahead,
        counts,
        fine_nodes,
        *arrived,
        gains,
    )
    parts = [parts[0]] + [shifted(parts[d], "gx", d, True) for d in range(1, members)]
    if members > 1:
        parts[1], coarse_sender, coarse_receiver, top_parent = lax.optimization_barrier(
            (parts[1], coarse_sender, coarse_receiver, top_parent)
        )
    share = jnp.concatenate(
        [coarse_sender.reshape(1, -1), coarse_receiver.reshape(1, -1), top_parent.reshape(1, -1)],
        axis=1,
    )
    mixed = [share] + [shifted(share, "gx", d, True) for d in range(1, members)]
    per = coarse_sender.shape[-1]
    senders = jnp.concatenate([piece[:, :per] for piece in mixed], axis=1)
    senders = lax.rem(me - senders // size + members, members) * size + lax.rem(senders, size)
    receivers = jnp.concatenate(
        [piece[:, per : 2 * per] + d * size for d, piece in enumerate(mixed)], axis=1
    )
    tops_of = jnp.concatenate([piece[:, 2 * per :] for piece in mixed], axis=1)

    (zero,) = call(
        functools.partial(mean_kernel, members),
        [shape((size, width), BF16)],
        LOOSE_SPEC,
        [LOOSE_SPEC] + [VMEM_SPEC] * (members - 1),
        [],
        *parts,
    )
    zeros = [zero] + [shifted(zero, "gx", d, True) for d in range(1, members)]

    chunk = min(COARSE_CHUNK, per * members, top_edges)
    fine_state, coarse_state = call(
        functools.partial(upper_kernel, members, chunk),
        [shape((nodes, width), BF16), shape((size, width), BF16)],
        HBM_SPEC,
        [HBM_SPEC] * 6 + [LOOSE_SPEC] * 4 + [VMEM_SPEC] + [LOOSE_SPEC] * 2 + [VMEM_SPEC] * (members - 1),
        [
            pltpu.VMEM((2 * (count + PAD), LANES), F32),
            pltpu.VMEM((2 * (count + PAD), LANES), F32),
            pltpu.VMEM((2 * (chunk + PAD), LANES), F32),
            pltpu.VMEM((2, chunk, width), BF16),
            pltpu.VMEM((count, width), F32),
            pltpu.VMEM((count, width), BF16),
            pltpu.VMEM((count, width), BF16),
            pltpu.VMEM((nodes, width), BF16),
            pltpu.SMEM((1, per * members), jnp.int32),
            pltpu.SMEM((1, per * members), jnp.int32),
            pltpu.SMEM((1, top_edges), jnp.int32),
            pltpu.SMEM((1, top_edges), jnp.int32),
            pltpu.VMEM(coarse_weights.shape, BF16),
            pltpu.VMEM(top_weights.shape, BF16),
            pltpu.SemaphoreType.DMA((6,)),
        ],
        senders,
        receivers,
        top_sender,
        top_receiver,
        coarse_weights,
        top_weights,
        receivers,
        top_receiver,
        tops_of,
        behind,
        fine_one,
        gains,
        *zeros,
    )
    return (fine_state, coarse_state[None])


def solution(mesh):
    placed = (
        P(("gx", "gy"), None),
        P(),
        P(),
        P(),
        P(),
        P("gx", "gy", None, None),
        P("gx", "gy", None),
        P("gx", "gy", None),
        P(("gx", "gy"), None),
        P(("gx", "gy")),
        P("gy", "gx"),
        P("gy", "gx"),
        P("gy", "gx"),
        P("gy", None),
        P("gy", None),
    )
    return jax.shard_map(
        body,
        mesh=mesh,
        in_specs=placed,
        out_specs=(P(("gx", "gy"), None), P("gy", "gx", None)),
        check_vma=False,
    )
```
